32 devices in a mesh: rows: 8 (over z, x), grp: 4 (over y, core).
Axes of the slice: x: 2, y: 2, z: 4, core: 2. Of those that a mesh axis runs over, the one named last changes fastest.
Arguments:
- user_features: bfloat16 [4, 2048, 256], P('grp', 'rows'), may hold values from -72 to 72
- w_first: bfloat16 [256, 256], replicated, may hold values from -0.375 to 0.375
- w_second: bfloat16 [256, 256], replicated, may hold values from -0.375 to 0.375
- item_embed: bfloat16 [4, 2048, 256], P('grp', 'rows'), may hold values from -27 to 27
- example_weight: float32 [4, 2048], P('grp', 'rows'), may hold values from 0.02 to 0.2
- positive: int32 [4, 2048], P('grp', 'rows'), may hold values from 0 to 2047
- item_owner: int32 [4, 2048, 1], P('grp', 'rows'), may hold values from 0 to 7; in each aligned block of 256 rows (0 to 255, 256 to 511, ..., all dimensions but the last counted through in order) at most 128 rows name the same one
- item_row: int32 [4, 2048], P('grp', 'rows'), may hold values from 0 to 4095
Outputs:
- grad_first: float32 [256, 256], replicated
- grad_second: float32 [256, 256], replicated
- grad_table: float32 [32768, 256], P('rows', 'grp')
The draws below stay inside these ranges and needn't reach their ends.
Inputs may be any that keep to these rules, and one draw needn't show every extreme that they name: `item_owner`: within the rows of one device (aligned blocks of 256 pairs of a group) no owner is named by more than 128 pairs, a bound that some block reaches.
All inputs are finite; a program needn't handle non-finite values.
Results may differ from the reference program's by a relative error of at most 0.0023.
The reference program's roundings to bfloat16 on the way count: a program that leaves them out, or rounds other values in their place, can miss the bound.
Values may be sent and summed in bfloat16 or wider, within the bound.
No kernel may reach another device: no remote copies, remote signals or barrier semaphores. Data moves between devices by JAX's collectives and lax.ppermute only.
A program may use at most 128 MiB of HBM per device.

```python
import math
import jax
import jax.numpy as jnp
import numpy as np
from jax import lax

D = 256
DIN = 256
DH = 256
BATCH_DEV = 256
ITEMS_DEV = 4096
GU = 2048
CAP = 128
N_ROWS = 8
N_GRP = 4


def draw_user_features(key, part):
    first_key = jax.random.fold_in(jax.random.fold_in(key, 11), 0)
    values = jnp.clip(jax.random.normal(first_key, (N_GRP, GU, DIN), jnp.float32), -6.0, 6.0)
    return values.astype(jnp.bfloat16)


def draw_item_embed(key, part):
    first_key = jax.random.fold_in(jax.random.fold_in(key, 23), 0)
    values = 0.15 * jnp.clip(jax.random.normal(first_key, (N_GRP, GU, D), jnp.float32), -6.0, 6.0)
    return values.astype(jnp.bfloat16)


def with_ends(entries, own_key, least, top_value):
    dims = entries.shape
    place = [jax.random.randint(jax.random.fold_in(own_key, axis), (), 0, dims[axis]) for axis in range(len(dims))]
    entries = entries.at[tuple(place)].set(least)
    longest = dims.index(max(dims))
    place[longest] = (place[longest] + 1) % dims[longest]
    return entries.at[tuple(place)].set(top_value)


def shard_levels(rng, dims, shards, low, largest):
    gain = 1.0
    for axis_at, shards_of in shards:
        draws = jax.random.uniform(jax.random.fold_in(jax.random.fold_in(rng, 6), axis_at), (shards_of,), jnp.float32, low / len(shards), largest / len(shards))
        gain = gain * jnp.repeat(jnp.exp(draws), dims[axis_at] // shards_of).reshape((-1,) + (1,) * (len(dims) - 1 - axis_at))
    return gain


def cumulative_ranks(number_of, slope):
    loads = [(1 << 20) // math.isqrt(standing ** slope) + 1 for standing in range(1, number_of + 1)]
    width = 1 + sum(loads) // (1 << 30)
    return np.cumsum(np.array([max(1, weight // width) for weight in loads]))


def ranked_ids(own_key, extent, amount, lean):
    listing = cumulative_ranks(amount, lean)
    pick = jax.random.randint(jax.random.fold_in(own_key, 1), extent, 0, int(listing[amount - 1]))
    standing = jnp.searchsorted(jnp.asarray(listing, jnp.int32), pick, side="right")
    return jax.random.permutation(jax.random.fold_in(own_key, 2), amount)[standing].astype(jnp.int32)


def assign_block(rng, own, number, rows, count, top, limit, skew):
    ranking = jax.random.permutation(rng, count)
    packed, common = shares(count, rows * top, limit, skew, True), shares(count, rows * top, limit, skew, False)
    places = jnp.arange(count)

    def named(tallies, rotation):
        used = int((tallies > 0).sum())
        fixed = max(1, used // 4)
        passed = fixed + (places - fixed + rotation * (used - fixed)) % max(1, count - fixed)
        return jnp.zeros((count,), jnp.int32).at[ranking[jnp.where(places < fixed, places, passed)]].set(jnp.asarray(tallies, jnp.int32))

    tallies = jnp.where(number % 4 == 0, named(packed, number // 4), named(common, number - number // 4 - 1))
    mixed = jax.random.permutation(jax.random.fold_in(own, 3), count)
    donor, sink = mixed[0:count // 2 * 2:2], mixed[1:count // 2 * 2:2]
    room = jnp.minimum(tallies[donor] - 1, limit - tallies[sink]) // 2
    room = jnp.where((donor == ranking[0]) | (sink == ranking[0]) | (tallies[sink] == 0), 0, jnp.maximum(room, 0))
    passed = jax.random.randint(jax.random.fold_in(own, 4), (count // 2,), 0, 1 << 20) % (room + 1)
    tallies = tallies.at[donor].add(-passed).at[sink].add(passed)
    labels = jnp.searchsorted(jnp.cumsum(tallies), jnp.arange(rows * top), side="right").astype(jnp.int32)
    grid = labels.reshape(top, rows).T
    grid = grid[jax.random.permutation(jax.random.fold_in(own, 1), rows)]
    rotation = jax.random.randint(jax.random.fold_in(own, 2), (rows, 1), 0, top)
    return jnp.take_along_axis(grid, (jnp.arange(top)[None, :] + rotation) % top, axis=1)


def shares(amount, total, reach, skew, full):
    portions = [(1 << 20) // math.isqrt(grade ** skew) + 1 for grade in range(1, amount + 1)]
    largest = reach if full else min(reach, max(-(-total // amount), total * portions[0] // sum(portions)))
    least = 1 if total - largest >= amount - 1 else 0
    counts, surplus = [largest] + [least] * (amount - 1), total - largest - least * (amount - 1)
    while surplus > 0:
        candidates = [i for i in range(1, amount) if counts[i] < largest] or [i for i in range(1, amount) if counts[i] < reach]
        pool, remaining = sum([portions[i] for i in candidates]), surplus
        for i in candidates:
            more = min(reach - counts[i], max(1, remaining * portions[i] // pool), surplus)
            counts[i] = counts[i] + more
            surplus = surplus - more
    return np.array(counts)


def centred(rng, dims, scale, reach, held_as=jnp.bfloat16):
    array = scale * jax.random.normal(rng, dims, jnp.float32)
    return jnp.clip(array, min=-reach, max=reach).astype(held_as)


def setup_inputs(seed: int = 0) -> dict:
    key_list = jax.random.split(jax.random.key(seed), 9)
    user_features = draw_user_features(jax.random.fold_in(key_list[8], 71), 0)
    w_first = centred(key_list[1], (DIN, DH), DIN ** -0.5, 0.375)
    w_second = centred(key_list[2], (DH, D), DH ** -0.5, 0.375)
    item_embed = draw_item_embed(jax.random.fold_in(key_list[8], 71), 0)
    example_weight = jnp.clip(jnp.exp(math.log(0.2) - 2.3025851 * jax.random.uniform(key_list[4], (N_GRP, GU), jnp.float32) ** shard_levels(key_list[4], (N_GRP, GU), ((0, 4), (1, 8)), -0.2, 0.2)), 0.02, 0.2)
    positive = with_ends(jax.random.randint(key_list[5], (N_GRP, GU), 0, GU), jax.random.fold_in(key_list[5], 1), 0, GU - 1).astype(jnp.int32)
    item_owner_keys = jax.random.split(jax.random.fold_in(key_list[6], 1), N_GRP * GU // BATCH_DEV)
    item_owner_turns = jax.random.permutation(jax.random.fold_in(key_list[6], 3), N_GRP * GU // BATCH_DEV)
    item_owner = jax.vmap(lambda own, number: assign_block(jax.random.fold_in(key_list[6], 2), own, number, BATCH_DEV, N_ROWS, 1, CAP, 2))(item_owner_keys, item_owner_turns).reshape((N_GRP, GU, 1))
    item_row = with_ends(ranked_ids(key_list[7], (N_GRP, GU), ITEMS_DEV, 2), jax.random.fold_in(key_list[7], 3), 0, ITEMS_DEV - 1).astype(jnp.int32)
    return dict(user_features=user_features, w_first=w_first, w_second=w_second, item_embed=item_embed, example_weight=example_weight, positive=positive, item_owner=item_owner, item_row=item_row)


def reference(user_features, w_first, w_second, item_embed, example_weight, positive, item_owner, item_row):
    group_users = user_features.shape[1]
    row_block = math.gcd(group_users, 1024)
    num_blocks = group_users // row_block

    def one_group(inputs):
        features, group_items, weights, targets = inputs
        pre_act = jnp.dot(features, w_first, preferred_element_type=jnp.float32)
        hidden = jax.nn.silu(pre_act).astype(jnp.bfloat16)
        user_vecs = jnp.dot(hidden, w_second, preferred_element_type=jnp.float32).astype(jnp.bfloat16)
        items_wide = group_items.astype(jnp.float32)
        users_wide = user_vecs.astype(jnp.float32)
        columns = jnp.arange(group_users, dtype=jnp.int32)

        def block_step(accum, block_no):
            first_row = (block_no * row_block).astype(jnp.int32)
            user_block = lax.dynamic_slice_in_dim(users_wide, first_row, row_block, 0)
            weight_block = lax.dynamic_slice_in_dim(weights, first_row, row_block, 0)
            target_block = lax.dynamic_slice_in_dim(targets, first_row, row_block, 0)
            scores = jnp.dot(user_block, items_wide.T)
            row_max = jnp.max(scores, axis=1, keepdims=True)
            log_total = row_max + jnp.log(jnp.sum(jnp.exp(scores - row_max), axis=1, keepdims=True))
            chosen = (columns[None, :] == target_block[:, None]).astype(jnp.float32)
            dscore = (weight_block[:, None] * (jnp.exp(scores - log_total) - chosen)).astype(jnp.bfloat16)
            dscore_wide = dscore.astype(jnp.float32)
            grad_block = jnp.dot(dscore_wide, items_wide)
            accum = accum + jnp.dot(dscore_wide.T, user_block)
            return accum, grad_block

        grad_item, grad_blocks = lax.scan(block_step, jnp.zeros((group_users, D), jnp.float32),
                                          jnp.arange(num_blocks, dtype=jnp.int32))
        grad_user = grad_blocks.reshape(group_users, D).astype(jnp.bfloat16)
        d_second = jnp.dot(hidden.T, grad_user, preferred_element_type=jnp.float32)
        back_grad = jnp.dot(grad_user, w_second.T, preferred_element_type=jnp.float32)
        sigmoid_pre = jax.nn.sigmoid(pre_act)
        grad_pre = (back_grad * sigmoid_pre * (1.0 + pre_act * (1.0 - sigmoid_pre))).astype(jnp.bfloat16)
        d_first = jnp.dot(features.T, grad_pre, preferred_element_type=jnp.float32)
        return grad_item, d_first, d_second

    grad_item, d_first, d_second = lax.map(one_group, (user_features, item_embed, example_weight, positive))
    grad_first = jnp.sum(d_first, axis=0)
    grad_second = jnp.sum(d_second, axis=0)
    table_ids = (item_owner[:, :, 0] * ITEMS_DEV + item_row).astype(jnp.int32)
    grad_table = jax.ops.segment_sum(grad_item.reshape(-1, D), table_ids.reshape(-1),
                                     num_segments=ITEMS_DEV * N_ROWS)
    return grad_first, grad_second, grad_table
```

```python
import functools

import jax
import jax.numpy as jnp
from jax import lax
from jax.experimental import pallas as pl
from jax.experimental.pallas import tpu as pltpu
from jax.sharding import PartitionSpec as P


ITEMS_DEV = 4096
META = 16
VMEM_BUDGET = 24 * 2**20
BF16 = jnp.bfloat16
F32 = jnp.float32


def dot_nn(left, right):
    return jnp.dot(left, right, preferred_element_type=F32)


def contract_first(left, right):
    return lax.dot_general(left, right, (((0,), (0,)), ((), ())), preferred_element_type=F32)


def contract_last(left, right):
    return lax.dot_general(left, right, (((1,), (1,)), ((), ())), preferred_element_type=F32)


def stack_rows(rows, width):
    line = lax.broadcasted_iota(jnp.int32, (META, width), 0)
    block = jnp.zeros((META, width), F32)
    for at, row in enumerate(rows):
        block = jnp.where(line == at, row, block)
    return block.astype(BF16)


def pack_kernel(
    weight_hbm, target_hbm, owner_hbm, row_hbm, meta_ref, weight_ref, target_ref, owner_ref, row_ref, sems
):
    moves = [
        (weight_hbm, weight_ref),
        (target_hbm, target_ref),
        (owner_hbm, owner_ref),
        (row_hbm, row_ref),
    ]
    copies = [pltpu.make_async_copy(*move, sems.at[at]) for at, move in enumerate(moves)]
    for copy in copies:
        copy.start()
    for copy in copies:
        copy.wait()
    weight = weight_ref[...]
    high = weight.astype(BF16).astype(F32)
    middle = (weight - high).astype(BF16).astype(F32)
    low = weight - high - middle
    rows = [owner_ref[...].astype(F32)]
    for digits in (row_ref[...], target_ref[...]):
        rows += [(digits >> 8).astype(F32), (digits & 255).astype(F32)]
    meta_ref[...] = stack_rows([*rows, high, middle, low], weight.shape[1])


def group_kernel(users, slots, begin, first, *refs):
    user_refs, refs = refs[:users], refs[users:]
    if first:
        item_refs, refs = refs[:slots], refs[slots:]
    else:
        items_ref, refs = refs[0], refs[1:]
    first_ref, second_ref = refs[:2]
    refs = refs[2:]
    if not first:
        mine_in, other_in = refs[2:4]
        refs = refs[4:]
    dscore_ref, vecs_ref, mine_ref, other_ref = refs[:4]
    refs = refs[4:]
    if first:
        items_ref, refs = refs[0], refs[1:]
    scores_refs = refs
    count = user_refs[0].shape[0] - META
    lanes = 128
    tall = 16
    me = lax.axis_index("rows")
    flip = lax.axis_index("grp") % 2 == 1
    if first:
        for slot in range(slots):
            items_ref[slot * count : (slot + 1) * count, :] = item_refs[slot][...]
    w_first = first_ref[...]
    w_second = second_ref[...]
    lane = lax.broadcasted_iota(jnp.int32, (tall, lanes), 1)

    def span(slot):
        return slice(slot * count, (slot + 1) * count)

    state = []
    for user in range(users):
        features = user_refs[user][0:count, :]
        meta = jnp.transpose(user_refs[user][count : count + META, :].astype(F32))
        weight = meta[:, 5:6] + meta[:, 6:7] + meta[:, 7:8]
        target = (meta[:, 3:4] * 256.0 + meta[:, 4:5]).astype(jnp.int32)
        pre_act = dot_nn(features, w_first)
        gate = jax.nn.sigmoid(pre_act)
        hidden = (pre_act * gate).astype(BF16)
        vecs = dot_nn(hidden, w_second).astype(BF16)
        vecs_ref[:, span(begin + user)] = jnp.transpose(vecs)
        state.append((weight, target, hidden, vecs))

    def score(user, slot):
        scores_refs[user][:, span(slot)] = contract_last(state[user][3], items_ref[span(slot), :])

    def soften(user, line):
        rows = slice(line * tall, (line + 1) * tall)
        weight = state[user][0][rows]
        away = lane - state[user][1][rows]
        total_lanes = slots * count
        parts = [scores_refs[user][rows, at : at + lanes] for at in range(0, total_lanes, lanes)]
        top = parts[0]
        for part in parts[1:]:
            top = jnp.maximum(top, part)
        top = jnp.max(top, axis=1, keepdims=True)
        parts = [jnp.exp(part - top) for part in parts]
        total = parts[0]
        for part in parts[1:]:
            total = total + part
        scale = weight / jnp.sum(total, axis=1, keepdims=True)
        for at, part in enumerate(parts):
            start = at * lanes
            base = (me ^ (start // count)) * count + start % count
            part = part * scale
            part = jnp.where(away == -base, part - weight, part)
            out = slice((begin + user) * count + line * tall, (begin + user) * count + (line + 1) * tall)
            dscore_ref[out, start : start + lanes] = part.astype(BF16)

    def pull(user):
        hidden = state[user][2]
        half = slots * count // 2
        grad_user = dot_nn(dscore_ref[span(begin + user), :half], items_ref[:half, :])
        grad_user += dot_nn(dscore_ref[span(begin + user), half:], items_ref[half:, :])
        grad_user = grad_user.astype(BF16)
        d_second = contract_first(hidden, grad_user)
        back = contract_last(grad_user, w_second)
        features = user_refs[user][0:count, :]
        pre_act = dot_nn(features, w_first)
        gate = jax.nn.sigmoid(pre_act)
        grad_pre = back * gate * (1.0 + pre_act * (1.0 - gate))
        d_first = contract_first(features, grad_pre.astype(BF16))
        return d_first, d_second

    lines = count // tall
    for slot in range(slots):
        score(0, slot)
    for user in range(users):
        for line in range(lines):
            soften(user, line)
            if user + 1 < users and line % (lines // slots) == 0:
                score(user + 1, line // (lines // slots))
    for user in range(users):
        d_first, d_second = pull(user)
        mine = jnp.where(flip, d_second, d_first)
        other = jnp.where(flip, d_first, d_second)
        if user:
            mine_ref[...] += mine
            other_ref[...] += other
        else:
            mine_ref[...] = mine if first else mine_in[...] + mine
            other_ref[...] = other if first else other_in[...] + other


def select_slots(meta_refs, cap):
    me = lax.axis_index("rows").astype(F32)
    count = meta_refs[0].shape[1]
    before = (
        lax.broadcasted_iota(jnp.int32, (count, count), 0)
        < lax.broadcasted_iota(jnp.int32, (count, count), 1)
    ).astype(F32).astype(BF16)
    place = lax.broadcasted_iota(jnp.int32, (cap, count), 0)
    picks = []
    for ref in meta_refs:
        meta = ref[...].astype(F32)
        owned = (meta == me).astype(F32)
        rank = dot_nn(owned.astype(BF16), before)[0:1].astype(jnp.int32)
        rank = jnp.where(owned[0:1] > 0.5, rank, -1)
        picks.append((place == rank).astype(F32).astype(BF16))
    return picks


def rows_kernel(cap, slots, *refs):
    metas, rows_ref = refs[:slots], refs[slots]
    picks = select_slots(metas, cap)
    for slot in range(slots):
        digits = contract_last(metas[slot][...], picks[slot])
        ones = contract_last(jnp.ones((META, picks[slot].shape[1]), BF16), picks[slot])
        row = digits[1:2] * 256.0 + digits[2:3]
        row = jnp.where(ones[0:1] > 0.5, row, -1.0)
        rows_ref[:, slot * cap : (slot + 1) * cap] = jnp.broadcast_to(row, (8, cap))


def compact_kernel(cap, slots, groups, steps, *refs):
    dscore_ref, vecs_ref, refs = refs[0], refs[1], refs[2:]
    metas, outs = refs[:slots], refs[slots:]
    picks = select_slots(metas, cap)
    count = metas[0].shape[1]
    width = vecs_ref.shape[0] // groups
    me = lax.axis_index("grp")
    blocks = [partner(me, step, groups) for step in steps]
    vecs = [vecs_ref[pl.ds(pl.multiple_of(one * width, width), width), :] for one in blocks]
    vecs = jnp.concatenate(vecs, axis=0)
    wide = min(2, slots)
    for slot in range(0, slots, wide):
        part = dot_nn(vecs, dscore_ref[:, slot * count : (slot + wide) * count]).astype(BF16)
        for one in range(wide):
            place = slice((slot + one) * cap, (slot + one + 1) * cap)
            packed = contract_last(part[:, one * count : (one + 1) * count], picks[slot + one])
            for at in range(len(steps)):
                outs[at][:, place] = packed[at * width : (at + 1) * width].astype(BF16)


def scatter_kernel(sources, first, *refs):
    grads, rows, out_ref = refs[:sources], refs[sources : 2 * sources], refs[-1]
    width, span = grads[0].shape
    low_size = 256
    high_size = out_ref.shape[1] // low_size
    line = lax.broadcasted_iota(jnp.int32, (low_size, span), 0).astype(F32)
    for source in range(sources):
        row = rows[source][0:1, :]
        high = jnp.floor(row / low_size)
        low = row - high * low_size
        onehot = (line == low).astype(F32).astype(BF16)
        grad = grads[source][...].astype(F32)
        left = jnp.concatenate(
            [jnp.where(high == part, grad, 0.0).astype(BF16) for part in range(high_size)], axis=0
        )
        result = contract_last(left, onehot)
        for part in range(high_size):
            spot = slice(part * low_size, (part + 1) * low_size)
            value = result[part * width : (part + 1) * width]
            if source:
                out_ref[:, spot] += value
            else:
                out_ref[:, spot] = value if first else refs[2 * sources][:, spot] + value


VMEM = pl.BlockSpec(memory_space=pltpu.VMEM)


def call(kernel, args, shapes, scratch=(), aliases=None, flops=1 << 20, limit=12):
    return pl.pallas_call(
        kernel,
        out_shape=shapes,
        in_specs=[VMEM] * len(args),
        out_specs=[VMEM] * len(shapes),
        scratch_shapes=list(scratch),
        input_output_aliases=aliases or {},
        compiler_params=pltpu.CompilerParams(vmem_limit_bytes=limit * 2**20),
        cost_estimate=pl.CostEstimate(flops=flops, bytes_accessed=1 << 20, transcendentals=0),
    )(*args)


def partner(me, step, groups):
    return me ^ step if groups & (groups - 1) == 0 else (me + step) % groups


def to_partner(value, step, groups):
    if step == 0:
        return value
    if groups & (groups - 1) == 0:
        pairs = [(one, one ^ step) for one in range(groups)]
    else:
        pairs = [(one, (one + step) % groups) for one in range(groups)]
    return lax.ppermute(value, "grp", pairs)


def along(value, bit, size):
    return lax.ppermute(value, "rows", [(one, one ^ bit) for one in range(size)])


def gather_slots(own, size, early=()):
    slots = [own]
    for slot in range(1, size):
        bit = slot & -slot
        if slot in early:
            bit = 1 << (slot.bit_length() - 1)
        slots.append(along(slots[slot ^ bit], bit, size))
    return slots


def sum_towers(mine, other, groups):
    if groups != 4:
        mine, other = lax.psum((mine, other), "grp")
        return mine, other
    flip = lax.axis_index("grp") % 2 == 1
    got = to_partner(other, 1, groups)
    half = mine + got
    got = to_partner(half, 2, groups)
    half = half + got
    rest = to_partner(half, 1, groups)
    return jnp.where(flip, rest, half), jnp.where(flip, half, rest)


def whole_group_body(*args):
    return whole_group_step(*args)


def whole_group_step(
    user_features, w_first, w_second, item_embed, example_weight, positive, item_owner, item_row
):
    peers, groups = lax.axis_size("rows"), lax.axis_size("grp")
    features, own_items = user_features[0], item_embed[0]
    count, width = own_items.shape
    cap = max(2, 4 * count // peers)
    batch = min(2, peers)
    args = [example_weight, positive, item_owner[:, :, 0], item_row]
    line = (1, count)
    meta = pl.pallas_call(
        pack_kernel,
        out_shape=jax.ShapeDtypeStruct((META, width), BF16),
        in_specs=[pl.BlockSpec(memory_space=pltpu.HBM)] * len(args),
        out_specs=VMEM,
        scratch_shapes=[
            pltpu.VMEM(line, F32),
            pltpu.VMEM(line, jnp.int32),
            pltpu.VMEM(line, jnp.int32),
            pltpu.VMEM(line, jnp.int32),
            pltpu.SemaphoreType.DMA((len(args),)),
        ],
        cost_estimate=pl.CostEstimate(flops=1 << 33, bytes_accessed=1 << 20, transcendentals=0),
    )(*args)
    users = jnp.concatenate([features, meta], axis=0)
    items = own_items
    item_slots = [items, *gather_slots(own_items, peers, early=(3,))[1:]]
    user_slots = gather_slots(users, peers, early=(3,))
    metas = [slot[count:] for slot in user_slots]
    rows = call(
        functools.partial(rows_kernel, cap, peers),
        metas,
        [jax.ShapeDtypeStruct((8, peers * cap), F32)],
    )[0]
    all_rows = [rows]
    for step in range(1, groups):
        all_rows.append(to_partner(rows, step, groups))
    tower = [jax.ShapeDtypeStruct((width, width), F32)] * 2
    pairs = peers * count
    state = []
    for step in range(peers // batch):
        first = step == 0
        args = user_slots[step * batch : (step + 1) * batch]
        args += item_slots if first else [gathered]
        args += [w_first, w_second, *state]
        at = len(args) - 4
        shapes = [
            jax.ShapeDtypeStruct((pairs, pairs), BF16),
            jax.ShapeDtypeStruct((width, pairs), BF16),
            *tower,
            *[jax.ShapeDtypeStruct((pairs, width), BF16)] * first,
        ]
        state = call(
            functools.partial(group_kernel, batch, peers, step * batch, first),
            args,
            shapes,
            scratch=[pltpu.VMEM((count, pairs), F32) for _ in range(batch)],
            aliases={} if first else {at + one: one for one in range(4)},
            flops=6 * batch * peers * count * count * width,
            limit=16,
        )
        if first:
            *state, gathered = state
    dscore, vecs, *state = state
    grad_first, grad_second = sum_towers(*state, groups)
    sends = []
    halves = [range(groups // 2, groups), range(groups // 2)]
    for steps in halves:
        outs = call(
            functools.partial(compact_kernel, cap, peers, groups, steps),
            [dscore, vecs, *metas],
            [jax.ShapeDtypeStruct((width // groups, peers * cap), BF16)] * len(steps),
            flops=pairs * pairs * width,
        )
        sends = [*outs, *sends]
    got = [sends[0]]
    for step in range(1, groups):
        got.append(to_partner(sends[step], step, groups))
    table = None
    turns = [range(groups // 2), *[range(one, one + 1) for one in range(groups // 2, groups)]]
    for turn, steps in enumerate(turns):
        args = [*[got[one] for one in steps], *[all_rows[one] for one in steps]]
        args += [] if turn == 0 else [table]
        table = call(
            functools.partial(scatter_kernel, len(steps), turn == 0),
            args,
            [jax.ShapeDtypeStruct((width // groups, ITEMS_DEV), F32)],
        )[0]
    return grad_first, grad_second, table.T


def sharded_group_body(
    user_features, w_first, w_second, item_embed, example_weight, positive, item_owner, item_row
):
    features = user_features[0]
    own_items = item_embed[0]
    weights = example_weight[0]
    targets = positive[0]
    owners = item_owner[0, :, 0]
    item_rows = item_row[0]
    my_users = features.shape[0]
    feature_width = own_items.shape[1]
    peers = lax.axis_size("rows")
    my_index = lax.axis_index("rows")
    pre_act = jnp.dot(features, w_first, preferred_element_type=jnp.float32)
    hidden = jax.nn.silu(pre_act).astype(jnp.bfloat16)
    user_vecs = jnp.dot(hidden, w_second, preferred_element_type=jnp.float32).astype(jnp.bfloat16)
    gathered = lax.all_gather(own_items, "rows", axis=0, tiled=True)
    group_users = gathered.shape[0]
    scores = contract_last(user_vecs, gathered)
    row_max = jnp.max(scores, axis=1, keepdims=True)
    log_total = row_max + jnp.log(jnp.sum(jnp.exp(scores - row_max), axis=1, keepdims=True))
    columns = lax.broadcasted_iota(jnp.int32, (1, group_users), 1)
    chosen = (columns == targets[:, None]).astype(jnp.float32)
    dscore = (weights[:, None] * (jnp.exp(scores - log_total) - chosen)).astype(jnp.bfloat16)
    grad_user = jnp.dot(dscore, gathered, preferred_element_type=jnp.float32).astype(jnp.bfloat16)
    everyone = lax.all_gather(user_vecs, "rows", axis=0, tiled=True)
    target_all, total_all, weight_all = (
        lax.all_gather(targets.astype(jnp.float32), "rows", axis=0, tiled=True),
        lax.all_gather(log_total[:, 0], "rows", axis=0, tiled=True),
        lax.all_gather(weights, "rows", axis=0, tiled=True),
    )
    back_scores = contract_last(everyone, own_items)
    own_columns = my_index * my_users + lax.broadcasted_iota(jnp.int32, (1, my_users), 1)
    hits = (own_columns == target_all.astype(jnp.int32)[:, None]).astype(jnp.float32)
    back_dscore = (weight_all[:, None] * (jnp.exp(back_scores - total_all[:, None]) - hits)).astype(
        jnp.bfloat16
    )
    grad_item = contract_first(back_dscore, everyone)
    d_second = contract_first(hidden, grad_user)
    back_grad = contract_last(grad_user, w_second)
    sigmoid_pre = jax.nn.sigmoid(pre_act)
    grad_pre = (back_grad * sigmoid_pre * (1.0 + pre_act * (1.0 - sigmoid_pre))).astype(
        jnp.bfloat16
    )
    d_first = contract_first(features, grad_pre)
    grad_first, grad_second = lax.psum((d_first, d_second), ("rows", "grp"))
    capacity = max(2, 4 * my_users // peers)
    member = (owners[:, None] == lax.broadcasted_iota(jnp.int32, (1, peers), 1)).astype(jnp.int32)
    before = jnp.cumsum(member, axis=0) - member
    slot_rank = jnp.sum(before * member, axis=1)
    slots = owners * capacity + slot_rank
    send_grad = jnp.zeros((peers * capacity, feature_width), jnp.float32).at[slots].set(grad_item)
    send_grad = send_grad.reshape(peers, capacity, feature_width)
    send_rows = (
        jnp.full((peers * capacity,), -1.0, jnp.float32)
        .at[slots]
        .set(item_rows.astype(jnp.float32))
    )
    got_grad, got_rows = (
        lax.all_to_all(send_grad, "rows", split_axis=0, concat_axis=0, tiled=True),
        lax.all_to_all(
            send_rows.reshape(peers, capacity), "rows", split_axis=0, concat_axis=0, tiled=True
        ),
    )
    table_rows = got_rows.reshape(-1).astype(jnp.int32)
    table_rows = jnp.where(table_rows >= 0, table_rows, ITEMS_DEV)
    dense_grad = (
        jnp.zeros((ITEMS_DEV, feature_width), jnp.float32)
        .at[table_rows]
        .add(got_grad.reshape(-1, feature_width), mode="drop")
    )
    grad_table = lax.psum_scatter(dense_grad, "grp", scatter_dimension=1, tiled=True)
    return (grad_first, grad_second, grad_table)


def solution(mesh):
    placed = (
        P("grp", "rows", None),
        P(),
        P(),
        P("grp", "rows", None),
        P("grp", "rows"),
        P("grp", "rows"),
        P("grp", "rows", None),
        P("grp", "rows"),
    )

    def body(*args):
        count, width = args[3].shape[1:]
        pairs = count * mesh.shape["rows"]
        held = pairs * (8 * count + 6 * width)
        fits = held <= VMEM_BUDGET and count == width == args[0].shape[2] and count <= 256
        return (whole_group_body if fits else sharded_group_body)(*args)

    return jax.shard_map(
        body, mesh=mesh, in_specs=placed, out_specs=(P(), P(), P("rows", "grp")), check_vma=False
    )
```

```python
import functools

import jax
import jax.numpy as jnp
from jax import lax
from jax.experimental import pallas as pl
from jax.experimental.pallas import tpu as pltpu
from jax.sharding import PartitionSpec as P


ITEMS_DEV = 4096
META = 16
VMEM_BUDGET = 24 * 2**20
BF16 = jnp.bfloat16
F32 = jnp.float32


def dot_nn(left, right):
    return jnp.dot(left, right, preferred_element_type=F32)


def contract_first(left, right):
    return lax.dot_general(left, right, (((0,), (0,)), ((), ())), preferred_element_type=F32)


def contract_last(left, right):
    return lax.dot_general(left, right, (((1,), (1,)), ((), ())), preferred_element_type=F32)


def stack_rows(rows, width):
    line = lax.broadcasted_iota(jnp.int32, (META, width), 0)
    block = jnp.zeros((META, width), F32)
    for at, row in enumerate(rows):
        block = jnp.where(line == at, row, block)
    return block.astype(BF16)


def pack_kernel(
    weight_hbm, target_hbm, owner_hbm, row_hbm, meta_ref, weight_ref, target_ref, owner_ref, row_ref, sems
):
    moves = [
        (weight_hbm, weight_ref),
        (target_hbm, target_ref),
        (owner_hbm, owner_ref),
        (row_hbm, row_ref),
    ]
    copies = [pltpu.make_async_copy(*move, sems.at[at]) for at, move in enumerate(moves)]
    for copy in copies:
        copy.start()
    for copy in copies:
        copy.wait()
    weight = weight_ref[...]
    high = weight.astype(BF16).astype(F32)
    middle = (weight - high).astype(BF16).astype(F32)
    low = weight - high - middle
    rows = [owner_ref[...].astype(F32)]
    for digits in (row_ref[...], target_ref[...]):
        rows += [(digits >> 8).astype(F32), (digits & 255).astype(F32)]
    meta_ref[...] = stack_rows([*rows, high, middle, low], weight.shape[1])


def group_kernel(users, slots, begin, first, last, *refs):
    user_refs, refs = refs[:users], refs[users:]
    if first:
        item_refs, refs = refs[:slots], refs[slots:]
    else:
        items_ref, refs = refs[0], refs[1:]
    first_ref, second_ref = refs[:2]
    refs = refs[2:]
    if not first:
        mine_in, other_in = refs[2:4]
        refs = refs[4:]
    dscore_ref, vecs_ref, mine_ref, other_ref = refs[:4]
    refs = refs[4:]
    if first:
        items_ref, refs = refs[0], refs[1:]
    scores_ref, slopes_ref, hidden_ref, sums_ref = refs
    count = user_refs[0].shape[0] - META
    lanes = 128
    tall = 16
    me = lax.axis_index("rows")
    flip = lax.axis_index("grp") % 2 == 1
    if first:
        for slot in range(slots):
            items_ref[slot * count : (slot + 1) * count, :] = item_refs[slot][...]
    w_first = first_ref[...]
    w_second = second_ref[...]
    lane = lax.broadcasted_iota(jnp.int32, (tall, lanes), 1)
    lines = count // tall
    stride = max(1, lines // slots)

    def span(slot):
        return slice(slot * count, (slot + 1) * count)

    state = [None] * users

    def enter(user):
        features = user_refs[user][0:count, :]
        meta = jnp.transpose(user_refs[user][count : count + META, :].astype(F32))
        weight = meta[:, 5:6] + meta[:, 6:7] + meta[:, 7:8]
        target = (meta[:, 3:4] * 256.0 + meta[:, 4:5]).astype(jnp.int32)
        pre_act = dot_nn(features, w_first)
        gate = jax.nn.sigmoid(pre_act)
        hidden = (pre_act * gate).astype(BF16)
        slopes_ref[user % 3] = gate * (1.0 + pre_act * (1.0 - gate))
        hidden_ref[user % 3] = hidden
        vecs = dot_nn(hidden, w_second).astype(BF16)
        vecs_ref[:, span(begin + user)] = jnp.transpose(vecs)
        state[user] = [weight, target, vecs, None]

    def score(user, slot):
        part = contract_last(state[user][2], items_ref[span(slot), :])
        scores_ref[user % 2, :, span(slot)] = part

    def soften(user, line):
        rows = slice(line * tall, (line + 1) * tall)
        weight = state[user][0][rows]
        away = lane - state[user][1][rows]
        total_lanes = slots * count
        parts = [scores_ref[user % 2, rows, at : at + lanes] for at in range(0, total_lanes, lanes)]
        top = parts[0]
        for part in parts[1:]:
            top = jnp.maximum(top, part)
        top = jnp.max(top, axis=1, keepdims=True)
        parts = [jnp.exp(part - top) for part in parts]
        total = parts[0]
        for part in parts[1:]:
            total = total + part
        scale = weight / jnp.sum(total, axis=1, keepdims=True)
        for at, part in enumerate(parts):
            start = at * lanes
            base = (me ^ (start // count)) * count + start % count
            part = part * scale
            part = jnp.where(away == -base, part - weight, part)
            out = slice((begin + user) * count + line * tall, (begin + user) * count + (line + 1) * tall)
            dscore_ref[out, start : start + lanes] = part.astype(BF16)

    def pull(user, piece):
        one = state[user]
        rows = span(begin + user)
        half = slots * count // 2
        if piece == 0:
            one[3] = dot_nn(dscore_ref[rows, :half], items_ref[:half, :])
        elif piece == 1:
            one[3] = (one[3] + dot_nn(dscore_ref[rows, half:], items_ref[half:, :])).astype(BF16)
        elif piece == 2:
            keep(second_sum, 1, user, contract_first(hidden_ref[user % 3], one[3]))
            one[3] = contract_last(one[3], w_second)
        else:
            grad_pre = (one[3] * slopes_ref[user % 3]).astype(BF16)
            keep(first_sum, 0, user, contract_first(user_refs[user][0:count, :], grad_pre))

    def keep(ref, index, user, value):
        if user:
            ref[...] += value
        else:
            ref[...] = value if first else (mine_in, other_in)[index][...] + value

    first_sum, second_sum = (mine_ref, other_ref) if not last else (sums_ref.at[0], sums_ref.at[1])
    for step in range(users + 2):
        if step < users:
            enter(step)
        for line in range(lines):
            if step < users and line % stride == 0 and line // stride < slots:
                score(step, line // stride)
            if 1 <= step <= users:
                soften(step - 1, line)
            if 2 <= step and line % (lines // 4) == 0:
                pull(step - 2, line // (lines // 4))
    if last:
        mine_ref[...] = jnp.where(flip, sums_ref[1], sums_ref[0])
        other_ref[...] = jnp.where(flip, sums_ref[0], sums_ref[1])


def select_slots(meta_refs, cap):
    me = lax.axis_index("rows").astype(F32)
    count = meta_refs[0].shape[1]
    before = (
        lax.broadcasted_iota(jnp.int32, (count, count), 0)
        < lax.broadcasted_iota(jnp.int32, (count, count), 1)
    ).astype(F32).astype(BF16)
    place = lax.broadcasted_iota(jnp.int32, (cap, count), 0)
    picks = []
    for ref in meta_refs:
        meta = ref[...].astype(F32)
        owned = (meta == me).astype(F32)
        rank = dot_nn(owned.astype(BF16), before)[0:1].astype(jnp.int32)
        rank = jnp.where(owned[0:1] > 0.5, rank, -1)
        picks.append((place == rank).astype(F32).astype(BF16))
    return picks


def compact_kernel(cap, slots, groups, steps, *refs):
    dscore_ref, vecs_ref, refs = refs[0], refs[1], refs[2:]
    metas, outs = refs[:slots], refs[slots:]
    picks = select_slots(metas, cap)
    if len(outs) > len(steps):
        for slot in range(slots):
            digits = contract_last(metas[slot][...], picks[slot])
            ones = contract_last(jnp.ones((META, picks[slot].shape[1]), BF16), picks[slot])
            row = digits[1:2] * 256.0 + digits[2:3]
            row = jnp.where(ones[0:1] > 0.5, row, -1.0)
            outs[-1][:, slot * cap : (slot + 1) * cap] = row
    count = metas[0].shape[1]
    width = vecs_ref.shape[0] // groups
    me = lax.axis_index("grp")
    blocks = [partner(me, step, groups) for step in steps]
    vecs = [vecs_ref[pl.ds(pl.multiple_of(one * width, width), width), :] for one in blocks]
    vecs = jnp.concatenate(vecs, axis=0)
    wide = min(2, slots)
    for slot in range(0, slots, wide):
        part = dot_nn(vecs, dscore_ref[:, slot * count : (slot + wide) * count]).astype(BF16)
        for one in range(wide):
            place = slice((slot + one) * cap, (slot + one + 1) * cap)
            packed = contract_last(part[:, one * count : (one + 1) * count], picks[slot + one])
            for at in range(len(steps)):
                outs[at][:, place] = packed[at * width : (at + 1) * width].astype(BF16)


def scatter_kernel(sources, first, *refs):
    grads, rows, out_ref = refs[:sources], refs[sources : 2 * sources], refs[-1]
    width, span = grads[0].shape
    low_size = 256
    high_size = out_ref.shape[1] // low_size
    line = lax.broadcasted_iota(jnp.int32, (low_size, span), 0).astype(F32)
    for source in range(sources):
        row = rows[source][0:1, :]
        high = jnp.floor(row / low_size)
        low = row - high * low_size
        onehot = (line == low).astype(F32).astype(BF16)
        grad = grads[source][...].astype(F32)
        left = jnp.concatenate(
            [jnp.where(high == part, grad, 0.0).astype(BF16) for part in range(high_size)], axis=0
        )
        result = contract_last(left, onehot)
        for part in range(high_size):
            spot = slice(part * low_size, (part + 1) * low_size)
            value = result[part * width : (part + 1) * width]
            if source:
                out_ref[:, spot] += value
            else:
                out_ref[:, spot] = value if first else refs[2 * sources][:, spot] + value


VMEM = pl.BlockSpec(memory_space=pltpu.VMEM)


def call(kernel, args, shapes, scratch=(), aliases=None, flops=1 << 20, limit=12):
    return pl.pallas_call(
        kernel,
        out_shape=shapes,
        in_specs=[VMEM] * len(args),
        out_specs=[VMEM] * len(shapes),
        scratch_shapes=list(scratch),
        input_output_aliases=aliases or {},
        compiler_params=pltpu.CompilerParams(vmem_limit_bytes=limit * 2**20),
        cost_estimate=pl.CostEstimate(flops=flops, bytes_accessed=1 << 20, transcendentals=0),
    )(*args)


def partner(me, step, groups):
    return me ^ step if groups & (groups - 1) == 0 else (me + step) % groups


def to_partner(value, step, groups):
    if step == 0:
        return value
    if groups & (groups - 1) == 0:
        pairs = [(one, one ^ step) for one in range(groups)]
    else:
        pairs = [(one, (one + step) % groups) for one in range(groups)]
    return lax.ppermute(value, "grp", pairs)


def along(value, bit, size):
    return lax.ppermute(value, "rows", [(one, one ^ bit) for one in range(size)])


def gather_slots(own, size):
    slots = [own]
    for slot in range(1, size):
        bit = slot & -slot
        if slot == 3:
            bit = 2
        slots.append(along(slots[slot ^ bit], bit, size))
    return slots


def sum_towers(mine, other, groups):
    if groups != 4:
        mine, other = lax.psum((mine, other), "grp")
        return mine, other
    flip = lax.axis_index("grp") % 2 == 1
    got = to_partner(other, 1, groups)
    half = mine + got
    got = to_partner(half, 2, groups)
    half = half + got
    rest = to_partner(half, 1, groups)
    return jnp.where(flip, rest, half), jnp.where(flip, half, rest)


def whole_group_body(*args):
    return whole_group_step(*args)


def whole_group_step(
    user_features, w_first, w_second, item_embed, example_weight, positive, item_owner, item_row
):
    peers, groups = lax.axis_size("rows"), lax.axis_size("grp")
    features, own_items = user_features[0], item_embed[0]
    count, width = own_items.shape
    cap = max(2, 4 * count // peers)
    batch = min(2, peers)
    args = [example_weight, positive, item_owner[:, :, 0], item_row]
    line = (1, count)
    meta = pl.pallas_call(
        pack_kernel,
        out_shape=jax.ShapeDtypeStruct((META, width), BF16),
        in_specs=[pl.BlockSpec(memory_space=pltpu.HBM)] * len(args),
        out_specs=VMEM,
        scratch_shapes=[
            pltpu.VMEM(line, F32),
            pltpu.VMEM(line, jnp.int32),
            pltpu.VMEM(line, jnp.int32),
            pltpu.VMEM(line, jnp.int32),
            pltpu.SemaphoreType.DMA((len(args),)),
        ],
        cost_estimate=pl.CostEstimate(flops=1 << 33, bytes_accessed=1 << 20, transcendentals=0),
    )(*args)
    users = jnp.concatenate([features, meta], axis=0)
    items = own_items
    item_slots = [items, *gather_slots(own_items, peers)[1:]]
    user_slots = gather_slots(users, peers)
    metas = [slot[count:] for slot in user_slots]
    tower = [jax.ShapeDtypeStruct((width, width), F32)] * 2
    pairs = peers * count
    state = []
    for step in range(peers // batch):
        first = step == 0
        args = user_slots[step * batch : (step + 1) * batch]
        args += item_slots if first else [gathered]
        args += [w_first, w_second, *state]
        at = len(args) - 4
        shapes = [
            jax.ShapeDtypeStruct((pairs, pairs), BF16),
            jax.ShapeDtypeStruct((width, pairs), BF16),
            *tower,
            *[jax.ShapeDtypeStruct((pairs, width), BF16)] * first,
        ]
        state = call(
            functools.partial(group_kernel, batch, peers, step * batch, first, (step + 1) * batch == peers),
            args,
            shapes,
            scratch=[
                pltpu.VMEM((2, count, pairs), F32),
                pltpu.VMEM((3, count, width), F32),
                pltpu.VMEM((3, count, width), BF16),
                pltpu.VMEM((2, width, width), F32),
            ],
            aliases={} if first else {at + one: one for one in range(4)},
            flops=6 * batch * peers * count * count * width,
            limit=16,
        )
        if first:
            *state, gathered = state
    dscore, vecs, *state = state
    grad_first, grad_second = sum_towers(*state, groups)
    sends = []
    halves = [range(groups // 2, groups), range(groups // 2)]
    for half, steps in enumerate(halves):
        outs = call(
            functools.partial(compact_kernel, cap, peers, groups, steps),
            [dscore, vecs, *metas],
            [jax.ShapeDtypeStruct((width // groups, peers * cap), BF16)] * len(steps)
            + [jax.ShapeDtypeStruct((1, peers * cap), F32)] * (half == 0),
            flops=pairs * pairs * width,
        )
        if half == 0:
            *outs, rows = outs
        sends = [*outs, *sends]
    all_rows = [rows]
    for step in range(1, groups):
        all_rows.append(to_partner(rows, step, groups))
    got = [sends[0]]
    for step in range(1, groups):
        got.append(to_partner(sends[step], step, groups))
    table = None
    turns = [range(groups // 2), *[range(one, one + 1) for one in range(groups // 2, groups)]]
    for turn, steps in enumerate(turns):
        args = [*[got[one] for one in steps], *[all_rows[one] for one in steps]]
        args += [] if turn == 0 else [table]
        table = call(
            functools.partial(scatter_kernel, len(steps), turn == 0),
            args,
            [jax.ShapeDtypeStruct((width // groups, ITEMS_DEV), F32)],
        )[0]
    return grad_first, grad_second, table.T


def sharded_group_body(
    user_features, w_first, w_second, item_embed, example_weight, positive, item_owner, item_row
):
    features = user_features[0]
    own_items = item_embed[0]
    weights = example_weight[0]
    targets = positive[0]
    owners = item_owner[0, :, 0]
    item_rows = item_row[0]
    my_users = features.shape[0]
    feature_width = own_items.shape[1]
    peers = lax.axis_size("rows")
    my_index = lax.axis_index("rows")
    pre_act = jnp.dot(features, w_first, preferred_element_type=jnp.float32)
    hidden = jax.nn.silu(pre_act).astype(jnp.bfloat16)
    user_vecs = jnp.dot(hidden, w_second, preferred_element_type=jnp.float32).astype(jnp.bfloat16)
    gathered = lax.all_gather(own_items, "rows", axis=0, tiled=True)
    group_users = gathered.shape[0]
    scores = contract_last(user_vecs, gathered)
    row_max = jnp.max(scores, axis=1, keepdims=True)
    log_total = row_max + jnp.log(jnp.sum(jnp.exp(scores - row_max), axis=1, keepdims=True))
    columns = lax.broadcasted_iota(jnp.int32, (1, group_users), 1)
    chosen = (columns == targets[:, None]).astype(jnp.float32)
    dscore = (weights[:, None] * (jnp.exp(scores - log_total) - chosen)).astype(jnp.bfloat16)
    grad_user = jnp.dot(dscore, gathered, preferred_element_type=jnp.float32).astype(jnp.bfloat16)
    everyone = lax.all_gather(user_vecs, "rows", axis=0, tiled=True)
    target_all, total_all, weight_all = (
        lax.all_gather(targets.astype(jnp.float32), "rows", axis=0, tiled=True),
        lax.all_gather(log_total[:, 0], "rows", axis=0, tiled=True),
        lax.all_gather(weights, "rows", axis=0, tiled=True),
    )
    back_scores = contract_last(everyone, own_items)
    own_columns = my_index * my_users + lax.broadcasted_iota(jnp.int32, (1, my_users), 1)
    hits = (own_columns == target_all.astype(jnp.int32)[:, None]).astype(jnp.float32)
    back_dscore = (weight_all[:, None] * (jnp.exp(back_scores - total_all[:, None]) - hits)).astype(
        jnp.bfloat16
    )
    grad_item = contract_first(back_dscore, everyone)
    d_second = contract_first(hidden, grad_user)
    back_grad = contract_last(grad_user, w_second)
    sigmoid_pre = jax.nn.sigmoid(pre_act)
    grad_pre = (back_grad * sigmoid_pre * (1.0 + pre_act * (1.0 - sigmoid_pre))).astype(
        jnp.bfloat16
    )
    d_first = contract_first(features, grad_pre)
    grad_first, grad_second = lax.psum((d_first, d_second), ("rows", "grp"))
    capacity = max(2, 4 * my_users // peers)
    member = (owners[:, None] == lax.broadcasted_iota(jnp.int32, (1, peers), 1)).astype(jnp.int32)
    before = jnp.cumsum(member, axis=0) - member
    slot_rank = jnp.sum(before * member, axis=1)
    slots = owners * capacity + slot_rank
    send_grad = jnp.zeros((peers * capacity, feature_width), jnp.float32).at[slots].set(grad_item)
    send_grad = send_grad.reshape(peers, capacity, feature_width)
    send_rows = (
        jnp.full((peers * capacity,), -1.0, jnp.float32)
        .at[slots]
        .set(item_rows.astype(jnp.float32))
    )
    got_grad, got_rows = (
        lax.all_to_all(send_grad, "rows", split_axis=0, concat_axis=0, tiled=True),
        lax.all_to_all(
            send_rows.reshape(peers, capacity), "rows", split_axis=0, concat_axis=0, tiled=True
        ),
    )
    table_rows = got_rows.reshape(-1).astype(jnp.int32)
    table_rows = jnp.where(table_rows >= 0, table_rows, ITEMS_DEV)
    dense_grad = (
        jnp.zeros((ITEMS_DEV, feature_width), jnp.float32)
        .at[table_rows]
        .add(got_grad.reshape(-1, feature_width), mode="drop")
    )
    grad_table = lax.psum_scatter(dense_grad, "grp", scatter_dimension=1, tiled=True)
    return (grad_first, grad_second, grad_table)


def solution(mesh):
    placed = (
        P("grp", "rows", None),
        P(),
        P(),
        P("grp", "rows", None),
        P("grp", "rows"),
        P("grp", "rows"),
        P("grp", "rows", None),
        P("grp", "rows"),
    )

    def body(*args):
        count, width = args[3].shape[1:]
        pairs = count * mesh.shape["rows"]
        held = pairs * (8 * count + 6 * width)
        fits = held <= VMEM_BUDGET and count == width == args[0].shape[2] and count <= 256
        return (whole_group_body if fits else sharded_group_body)(*args)

    return jax.shard_map(
        body, mesh=mesh, in_specs=placed, out_specs=(P(), P(), P("rows", "grp")), check_vma=False
    )
```

```python
import functools

import jax
import jax.numpy as jnp
from jax import lax
from jax.experimental import pallas as pl
from jax.experimental.pallas import tpu as pltpu
from jax.sharding import PartitionSpec as P


ITEMS_DEV = 4096
META = 16
VMEM_BUDGET = 24 * 2**20
BF16 = jnp.bfloat16
F32 = jnp.float32


def dot_nn(left, right):
    return jnp.dot(left, right, preferred_element_type=F32)


def contract_first(left, right):
    return lax.dot_general(left, right, (((0,), (0,)), ((), ())), preferred_element_type=F32)


def contract_last(left, right):
    return lax.dot_general(left, right, (((1,), (1,)), ((), ())), preferred_element_type=F32)


def stack_rows(rows, width):
    line = lax.broadcasted_iota(jnp.int32, (META, width), 0)
    block = jnp.zeros((META, width), F32)
    for at, row in enumerate(rows):
        block = jnp.where(line == at, row, block)
    return block.astype(BF16)


def pack_kernel(
    weight_hbm, target_hbm, owner_hbm, row_hbm, meta_ref, weight_ref, target_ref, owner_ref, row_ref, sems
):
    moves = [
        (weight_hbm, weight_ref),
        (target_hbm, target_ref),
        (owner_hbm, owner_ref),
        (row_hbm, row_ref),
    ]
    copies = [pltpu.make_async_copy(*move, sems.at[at]) for at, move in enumerate(moves)]
    for copy in copies:
        copy.start()
    for copy in copies:
        copy.wait()
    weight = weight_ref[...]
    high = weight.astype(BF16).astype(F32)
    middle = (weight - high).astype(BF16).astype(F32)
    low = weight - high - middle
    rows = [owner_ref[...].astype(F32)]
    for digits in (row_ref[...], target_ref[...]):
        rows += [(digits >> 8).astype(F32), (digits & 255).astype(F32)]
    meta_ref[...] = stack_rows([*rows, high, middle, low], weight.shape[1])


def group_kernel(users, slots, begin, first, last, *refs):
    user_refs, refs = refs[:users], refs[users:]
    if first:
        item_refs, refs = refs[:slots], refs[slots:]
    else:
        items_ref, refs = refs[0], refs[1:]
    first_ref, second_ref = refs[:2]
    refs = refs[2:]
    if not first:
        mine_in, other_in = refs[2:4]
        refs = refs[4:]
    dscore_ref, vecs_ref, mine_ref, other_ref = refs[:4]
    refs = refs[4:]
    if first:
        items_ref, refs = refs[0], refs[1:]
    scores_ref, slopes_ref, hidden_ref, sums_ref, weight_ref, target_ref, held_ref, grad_ref = refs
    count = user_refs[0].shape[0] - META
    lanes = 128
    tall = 16
    me = lax.axis_index("rows")
    flip = lax.axis_index("grp") % 2 == 1
    if first:
        for slot in range(slots):
            items_ref[slot * count : (slot + 1) * count, :] = item_refs[slot][...]
    w_first = first_ref[...]
    w_second = second_ref[...]
    lines = count // tall

    def span(slot):
        return slice(slot * count, (slot + 1) * count)

    wide = 4
    turns = lines // wide
    chunk = slots * count // turns

    def enter(user):
        features = user_refs[user][0:count, :]
        meta = jnp.transpose(user_refs[user][count : count + META, :].astype(F32))
        weight = meta[:, 5:6] + meta[:, 6:7] + meta[:, 7:8]
        target = (meta[:, 3:4] * 256.0 + meta[:, 4:5]).astype(jnp.int32)
        weight_ref[user] = jnp.broadcast_to(weight, (count, lanes))
        target_ref[user] = lax.broadcasted_iota(jnp.int32, (count, lanes), 1) - target
        pre_act = dot_nn(features, w_first)
        gate = jax.nn.sigmoid(pre_act)
        hidden = (pre_act * gate).astype(BF16)
        slopes_ref[user] = gate * (1.0 + pre_act * (1.0 - gate))
        hidden_ref[user] = hidden
        vecs = dot_nn(hidden, w_second).astype(BF16)
        vecs_ref[:, span(begin + user)] = jnp.transpose(vecs)
        held_ref[user] = vecs

    def score(user, turn):
        spot = pl.ds(turn * chunk, chunk)
        scores_ref[user, :, spot] = contract_last(held_ref[user], items_ref[spot, :])

    def soften(user, line):
        rows = pl.ds(line * tall, tall)
        weight = weight_ref[user, rows, :]
        away = target_ref[user, rows, :]
        total_lanes = slots * count
        parts = [scores_ref[user, rows, at : at + lanes] for at in range(0, total_lanes, lanes)]
        top = parts[0]
        for part in parts[1:]:
            top = jnp.maximum(top, part)
        top = jnp.max(top, axis=1, keepdims=True)
        parts = [jnp.exp(part - top) for part in parts]
        total = parts[0]
        for part in parts[1:]:
            total = total + part
        scale = weight / jnp.sum(total, axis=1, keepdims=True)
        for at, part in enumerate(parts):
            start = at * lanes
            base = (me ^ (start // count)) * count + start % count
            part = part * scale
            part = jnp.where(away == -base, part - weight, part)
            out = pl.ds((begin + user) * count + line * tall, tall)
            dscore_ref[out, start : start + lanes] = part.astype(BF16)

    def gather_grad(user, turn):
        spot = pl.ds(turn * chunk, chunk)
        term = dot_nn(dscore_ref[span(begin + user), spot], items_ref[spot, :])
        grad_ref[user] = grad_ref[user] + term

    def pull(user):
        grad_user = grad_ref[user].astype(BF16)
        keep(second_sum, 1, user, contract_first(hidden_ref[user], grad_user))
        grad_pre = (contract_last(grad_user, w_second) * slopes_ref[user]).astype(BF16)
        keep(first_sum, 0, user, contract_first(user_refs[user][0:count, :], grad_pre))

    def keep(ref, index, user, value):
        if user:
            ref[...] += value
        else:
            ref[...] = value if first else (mine_in, other_in)[index][...] + value

    first_sum, second_sum = (mine_ref, other_ref) if not last else (sums_ref.at[0], sums_ref.at[1])
    for user in range(users):
        enter(user)
        grad_ref[user] = jnp.zeros_like(grad_ref[user])
    for turn in range(turns):
        score(0, turn)
    for user in range(users):

        def body(turn, carry):
            if user + 1 < users:
                score(user + 1, turn)
            if user:
                gather_grad(user - 1, turn)
            for line in range(wide):
                soften(user, turn * wide + line)
            return carry

        for turn in range(turns):
            body(turn, 0)
    for turn in range(turns):
        gather_grad(users - 1, turn)
    for user in range(users):
        pull(user)
    if last:
        mine_ref[...] = jnp.where(flip, sums_ref[1], sums_ref[0])
        other_ref[...] = jnp.where(flip, sums_ref[0], sums_ref[1])


def select_slots(meta_refs, cap):
    me = lax.axis_index("rows").astype(F32)
    count = meta_refs[0].shape[1]
    before = (
        lax.broadcasted_iota(jnp.int32, (count, count), 0)
        < lax.broadcasted_iota(jnp.int32, (count, count), 1)
    ).astype(F32).astype(BF16)
    place = lax.broadcasted_iota(jnp.int32, (cap, count), 0)
    picks = []
    for ref in meta_refs:
        meta = ref[...].astype(F32)
        owned = (meta == me).astype(F32)
        rank = dot_nn(owned.astype(BF16), before)[0:1].astype(jnp.int32)
        rank = jnp.where(owned[0:1] > 0.5, rank, -1)
        picks.append((place == rank).astype(F32).astype(BF16))
    return picks


def compact_kernel(cap, slots, groups, steps, *refs):
    dscore_ref, vecs_ref, refs = refs[0], refs[1], refs[2:]
    metas, outs = refs[:slots], refs[slots:]
    picks = select_slots(metas, cap)
    if len(outs) > len(steps):
        for slot in range(slots):
            digits = contract_last(metas[slot][...], picks[slot])
            ones = contract_last(jnp.ones((META, picks[slot].shape[1]), BF16), picks[slot])
            row = digits[1:2] * 256.0 + digits[2:3]
            row = jnp.where(ones[0:1] > 0.5, row, -1.0)
            outs[-1][:, slot * cap : (slot + 1) * cap] = row
    count = metas[0].shape[1]
    width = vecs_ref.shape[0] // groups
    me = lax.axis_index("grp")
    blocks = [partner(me, step, groups) for step in steps]
    vecs = [vecs_ref[pl.ds(pl.multiple_of(one * width, width), width), :] for one in blocks]
    vecs = jnp.concatenate(vecs, axis=0)
    wide = min(2, slots)
    for slot in range(0, slots, wide):
        part = dot_nn(vecs, dscore_ref[:, slot * count : (slot + wide) * count]).astype(BF16)
        for one in range(wide):
            place = slice((slot + one) * cap, (slot + one + 1) * cap)
            packed = contract_last(part[:, one * count : (one + 1) * count], picks[slot + one])
            for at in range(len(steps)):
                outs[at][:, place] = packed[at * width : (at + 1) * width].astype(BF16)


def scatter_kernel(sources, first, *refs):
    grads, rows, out_ref = refs[:sources], refs[sources : 2 * sources], refs[-1]
    width, span = grads[0].shape
    low_size = 256
    high_size = out_ref.shape[1] // low_size
    line = lax.broadcasted_iota(jnp.int32, (low_size, span), 0).astype(F32)
    for source in range(sources):
        row = rows[source][0:1, :]
        high = jnp.floor(row / low_size)
        low = row - high * low_size
        onehot = (line == low).astype(F32).astype(BF16)
        grad = grads[source][...].astype(F32)
        left = jnp.concatenate(
            [jnp.where(high == part, grad, 0.0).astype(BF16) for part in range(high_size)], axis=0
        )
        result = contract_last(left, onehot)
        for part in range(high_size):
            spot = slice(part * low_size, (part + 1) * low_size)
            value = result[part * width : (part + 1) * width]
            if source:
                out_ref[:, spot] += value
            else:
                out_ref[:, spot] = value if first else refs[2 * sources][:, spot] + value


VMEM = pl.BlockSpec(memory_space=pltpu.VMEM)


def call(kernel, args, shapes, scratch=(), aliases=None, flops=1 << 20, limit=12):
    return pl.pallas_call(
        kernel,
        out_shape=shapes,
        in_specs=[VMEM] * len(args),
        out_specs=[VMEM] * len(shapes),
        scratch_shapes=list(scratch),
        input_output_aliases=aliases or {},
        compiler_params=pltpu.CompilerParams(vmem_limit_bytes=limit * 2**20),
        cost_estimate=pl.CostEstimate(flops=flops, bytes_accessed=1 << 20, transcendentals=0),
    )(*args)


def partner(me, step, groups):
    return me ^ step if groups & (groups - 1) == 0 else (me + step) % groups


def to_partner(value, step, groups):
    if step == 0:
        return value
    if groups & (groups - 1) == 0:
        pairs = [(one, one ^ step) for one in range(groups)]
    else:
        pairs = [(one, (one + step) % groups) for one in range(groups)]
    return lax.ppermute(value, "grp", pairs)


def along(value, bit, size):
    return lax.ppermute(value, "rows", [(one, one ^ bit) for one in range(size)])


def gather_slots(own, size):
    slots = [own]
    for slot in range(1, size):
        bit = slot & -slot
        if slot == 3:
            bit = 2
        slots.append(along(slots[slot ^ bit], bit, size))
    return slots


def sum_towers(mine, other, groups):
    if groups != 4:
        mine, other = lax.psum((mine, other), "grp")
        return mine, other
    flip = lax.axis_index("grp") % 2 == 1
    got = to_partner(other, 1, groups)
    half = mine + got
    got = to_partner(half, 2, groups)
    half = half + got
    rest = to_partner(half, 1, groups)
    return jnp.where(flip, rest, half), jnp.where(flip, half, rest)


def whole_group_body(*args):
    return whole_group_step(*args)


def whole_group_step(
    user_features, w_first, w_second, item_embed, example_weight, positive, item_owner, item_row
):
    peers, groups = lax.axis_size("rows"), lax.axis_size("grp")
    features, own_items = user_features[0], item_embed[0]
    count, width = own_items.shape
    cap = max(2, 4 * count // peers)
    batch = min(2, peers)
    args = [example_weight, positive, item_owner[:, :, 0], item_row]
    line = (1, count)
    meta = pl.pallas_call(
        pack_kernel,
        out_shape=jax.ShapeDtypeStruct((META, width), BF16),
        in_specs=[pl.BlockSpec(memory_space=pltpu.HBM)] * len(args),
        out_specs=VMEM,
        scratch_shapes=[
            pltpu.VMEM(line, F32),
            pltpu.VMEM(line, jnp.int32),
            pltpu.VMEM(line, jnp.int32),
            pltpu.VMEM(line, jnp.int32),
            pltpu.SemaphoreType.DMA((len(args),)),
        ],
        cost_estimate=pl.CostEstimate(flops=1 << 33, bytes_accessed=1 << 20, transcendentals=0),
    )(*args)
    users = jnp.concatenate([features, meta], axis=0)
    items = own_items
    item_slots = [items, *gather_slots(own_items, peers)[1:]]
    user_slots = gather_slots(users, peers)
    metas = [slot[count:] for slot in user_slots]
    tower = [jax.ShapeDtypeStruct((width, width), F32)] * 2
    pairs = peers * count
    state = []
    for step in range(peers // batch):
        first = step == 0
        args = user_slots[step * batch : (step + 1) * batch]
        args += item_slots if first else [gathered]
        args += [w_first, w_second, *state]
        at = len(args) - 4
        shapes = [
            jax.ShapeDtypeStruct((pairs, pairs), BF16),
            jax.ShapeDtypeStruct((width, pairs), BF16),
            *tower,
            *[jax.ShapeDtypeStruct((pairs, width), BF16)] * first,
        ]
        state = call(
            functools.partial(group_kernel, batch, peers, step * batch, first, (step + 1) * batch == peers),
            args,
            shapes,
            scratch=[
                pltpu.VMEM((batch, count, pairs), F32),
                pltpu.VMEM((batch, count, width), F32),
                pltpu.VMEM((batch, count, width), BF16),
                pltpu.VMEM((2, width, width), F32),
                pltpu.VMEM((batch, count, 128), F32),
                pltpu.VMEM((batch, count, 128), jnp.int32),
                pltpu.VMEM((batch, count, width), BF16),
                pltpu.VMEM((batch, count, width), F32),
            ],
            aliases={} if first else {at + one: one for one in range(4)},
            flops=6 * batch * peers * count * count * width,
            limit=16,
        )
        if first:
            *state, gathered = state
    dscore, vecs, *state = state
    grad_first, grad_second = sum_towers(*state, groups)
    sends = []
    halves = [range(groups // 2, groups), range(groups // 2)]
    for half, steps in enumerate(halves):
        outs = call(
            functools.partial(compact_kernel, cap, peers, groups, steps),
            [dscore, vecs, *metas],
            [jax.ShapeDtypeStruct((width // groups, peers * cap), BF16)] * len(steps)
            + [jax.ShapeDtypeStruct((1, peers * cap), F32)] * (half == 0),
            flops=pairs * pairs * width,
        )
        if half == 0:
            *outs, rows = outs
        sends = [*outs, *sends]
    all_rows = [rows]
    for step in range(1, groups):
        all_rows.append(to_partner(rows, step, groups))
    got = [sends[0]]
    for step in range(1, groups):
        got.append(to_partner(sends[step], step, groups))
    table = None
    turns = [range(groups // 2), *[range(one, one + 1) for one in range(groups // 2, groups)]]
    for turn, steps in enumerate(turns):
        args = [*[got[one] for one in steps], *[all_rows[one] for one in steps]]
        args += [] if turn == 0 else [table]
        table = call(
            functools.partial(scatter_kernel, len(steps), turn == 0),
            args,
            [jax.ShapeDtypeStruct((width // groups, ITEMS_DEV), F32)],
        )[0]
    return grad_first, grad_second, table.T


def sharded_group_body(
    user_features, w_first, w_second, item_embed, example_weight, positive, item_owner, item_row
):
    features = user_features[0]
    own_items = item_embed[0]
    weights = example_weight[0]
    targets = positive[0]
    owners = item_owner[0, :, 0]
    item_rows = item_row[0]
    my_users = features.shape[0]
    feature_width = own_items.shape[1]
    peers = lax.axis_size("rows")
    my_index = lax.axis_index("rows")
    pre_act = jnp.dot(features, w_first, preferred_element_type=jnp.float32)
    hidden = jax.nn.silu(pre_act).astype(jnp.bfloat16)
    user_vecs = jnp.dot(hidden, w_second, preferred_element_type=jnp.float32).astype(jnp.bfloat16)
    gathered = lax.all_gather(own_items, "rows", axis=0, tiled=True)
    group_users = gathered.shape[0]
    scores = contract_last(user_vecs, gathered)
    row_max = jnp.max(scores, axis=1, keepdims=True)
    log_total = row_max + jnp.log(jnp.sum(jnp.exp(scores - row_max), axis=1, keepdims=True))
    columns = lax.broadcasted_iota(jnp.int32, (1, group_users), 1)
    chosen = (columns == targets[:, None]).astype(jnp.float32)
    dscore = (weights[:, None] * (jnp.exp(scores - log_total) - chosen)).astype(jnp.bfloat16)
    grad_user = jnp.dot(dscore, gathered, preferred_element_type=jnp.float32).astype(jnp.bfloat16)
    everyone = lax.all_gather(user_vecs, "rows", axis=0, tiled=True)
    target_all, total_all, weight_all = (
        lax.all_gather(targets.astype(jnp.float32), "rows", axis=0, tiled=True),
        lax.all_gather(log_total[:, 0], "rows", axis=0, tiled=True),
        lax.all_gather(weights, "rows", axis=0, tiled=True),
    )
    back_scores = contract_last(everyone, own_items)
    own_columns = my_index * my_users + lax.broadcasted_iota(jnp.int32, (1, my_users), 1)
    hits = (own_columns == target_all.astype(jnp.int32)[:, None]).astype(jnp.float32)
    back_dscore = (weight_all[:, None] * (jnp.exp(back_scores - total_all[:, None]) - hits)).astype(
        jnp.bfloat16
    )
    grad_item = contract_first(back_dscore, everyone)
    d_second = contract_first(hidden, grad_user)
    back_grad = contract_last(grad_user, w_second)
    sigmoid_pre = jax.nn.sigmoid(pre_act)
    grad_pre = (back_grad * sigmoid_pre * (1.0 + pre_act * (1.0 - sigmoid_pre))).astype(
        jnp.bfloat16
    )
    d_first = contract_first(features, grad_pre)
    grad_first, grad_second = lax.psum((d_first, d_second), ("rows", "grp"))
    capacity = max(2, 4 * my_users // peers)
    member = (owners[:, None] == lax.broadcasted_iota(jnp.int32, (1, peers), 1)).astype(jnp.int32)
    before = jnp.cumsum(member, axis=0) - member
    slot_rank = jnp.sum(before * member, axis=1)
    slots = owners * capacity + slot_rank
    send_grad = jnp.zeros((peers * capacity, feature_width), jnp.float32).at[slots].set(grad_item)
    send_grad = send_grad.reshape(peers, capacity, feature_width)
    send_rows = (
        jnp.full((peers * capacity,), -1.0, jnp.float32)
        .at[slots]
        .set(item_rows.astype(jnp.float32))
    )
    got_grad, got_rows = (
        lax.all_to_all(send_grad, "rows", split_axis=0, concat_axis=0, tiled=True),
        lax.all_to_all(
            send_rows.reshape(peers, capacity), "rows", split_axis=0, concat_axis=0, tiled=True
        ),
    )
    table_rows = got_rows.reshape(-1).astype(jnp.int32)
    table_rows = jnp.where(table_rows >= 0, table_rows, ITEMS_DEV)
    dense_grad = (
        jnp.zeros((ITEMS_DEV, feature_width), jnp.float32)
        .at[table_rows]
        .add(got_grad.reshape(-1, feature_width), mode="drop")
    )
    grad_table = lax.psum_scatter(dense_grad, "grp", scatter_dimension=1, tiled=True)
    return (grad_first, grad_second, grad_table)


def solution(mesh):
    placed = (
        P("grp", "rows", None),
        P(),
        P(),
        P("grp", "rows", None),
        P("grp", "rows"),
        P("grp", "rows"),
        P("grp", "rows", None),
        P("grp", "rows"),
    )

    def body(*args):
        count, width = args[3].shape[1:]
        pairs = count * mesh.shape["rows"]
        held = pairs * (8 * count + 6 * width)
        fits = held <= VMEM_BUDGET and count == width == args[0].shape[2] and count <= 256
        return (whole_group_body if fits else sharded_group_body)(*args)

    return jax.shard_map(
        body, mesh=mesh, in_specs=placed, out_specs=(P(), P(), P("rows", "grp")), check_vma=False
    )
```
